256 devices in a mesh: dp: 8 (over z), feat: 32 (over x, y, core).
Axes of the slice: x: 4, y: 4, z: 8, core: 2. Of those that a mesh axis runs over, the one named last changes fastest.
Arguments:
- features: float32 [8192, 32768], P('dp', 'feat'), may hold values from -0.03125 to 0.03125
- labels: int32 [8192], P('dp'), may hold values from -1 to 1, as said below
- weights: float32 [32768], P('feat'), may hold values from -6 to 6
Outputs:
- gradient: float32 [32768], P('feat')
- newton_step: float32 [32768], P('feat')
- residual: float32 [32768], P('feat')
The draws below stay inside these ranges and needn't reach their ends.
Inputs may be any that keep to these rules, and one draw needn't show every extreme that they name: `labels`: every label is -1 or +1.
All inputs are finite; a program needn't handle non-finite values.
Results may differ from the reference program's by a relative error of at most 0.0003.
Values sent between devices are 32-bit elements; how exact they have to be, the bound alone decides.
A program may use at most 64 MiB of HBM per device.

```python
import jax
import jax.numpy as jnp
from jax import lax

CG_STEPS = 3
SAMPLES = 8192
FEATURES = 32768


def draw_labels(key, part):
    return (2 * jax.random.randint(jax.random.fold_in(key, 11), (SAMPLES,), 0, 2) - 1).astype(jnp.int32)


def steps_of(own_key, shape, cuts, smallest, high):
    def one(axis_at, blocks):
        steps = jax.random.uniform(jax.random.fold_in(jax.random.fold_in(own_key, 6), axis_at), (blocks,), jnp.float32, smallest / len(cuts), high / len(cuts))
        return jnp.repeat(jnp.exp(steps), shape[axis_at] // blocks).reshape((-1,) + (1,) * (len(shape) - axis_at - 1))

    level = one(*cuts[0])
    for cut in cuts[1:]:
        level = level * one(*cut)
    return level


def centred(stream_key, extent, scale, reach, shards=(), dtype=jnp.bfloat16):
    values = jax.random.normal(stream_key, extent, jnp.float32) * scale
    if len(shards) > 0:
        values = steps_of(stream_key, extent, shards, -0.22, 0.18) * values
    return jnp.clip(values, min=-reach, max=reach).astype(dtype)


def setup_inputs(seed: int = 0) -> dict:
    seeds = jax.random.split(jax.random.key(seed), 4)
    return {
        "features": centred(seeds[0], (SAMPLES, FEATURES), FEATURES ** -0.5, 0.03125, ((0, 8), (1, 32)), jnp.float32),
        "labels": draw_labels(jax.random.fold_in(seeds[3], 71), 0),
        "weights": centred(seeds[2], (FEATURES,), 1.0, 6.0, ((0, 32),), jnp.float32),
    }


PENALTY = 4.0


def reference(features, labels, weights):
    hi = lax.Precision.HIGHEST
    y = labels.astype(jnp.float32)
    margin = y * jnp.dot(features, weights, precision=hi)
    sig = 1.0 / (1.0 + jnp.exp(-margin))
    gradient = weights + PENALTY * jnp.dot((sig - 1.0) * y, features, precision=hi)
    curv = PENALTY * sig * (1.0 - sig)
    newton_step = jnp.zeros_like(weights)
    residual = -gradient
    direction = residual
    rr = jnp.sum(residual * residual)
    for step in range(CG_STEPS):
        image = direction + jnp.dot(curv * jnp.dot(features, direction, precision=hi), features, precision=hi)
        alpha = rr / jnp.sum(direction * image)
        newton_step = newton_step + alpha * direction
        residual = residual - alpha * image
        fresh = jnp.sum(residual * residual)
        direction = residual + (fresh / rr) * direction
        rr = fresh
    return gradient, newton_step, residual
```

```python
import functools

import jax
import jax.numpy as jnp
from jax import lax
from jax.experimental import pallas as pl
from jax.experimental.pallas import tpu as pltpu
from jax.sharding import PartitionSpec as P

CG_STEPS = 3
PENALTY = 4.0
MESH = pl.DeviceIdType.MESH

N = 1024
LANES = 128
ROWS = N // LANES
CHUNK = 256
NCHUNK = N // CHUNK
NX, NY, NC, NZ = 4, 4, 2, 8
NF = NX * NY * NC
SLOT = 16


def ring(d, n):
    return min(d, n - d)


F_PEERS = sorted(
    ((a, b, c) for a in range(NX) for b in range(NY) for c in range(NC) if (a, b, c) != (0, 0, 0)),
    key=lambda o: (-(ring(o[0], NX) + ring(o[1], NY)), -o[2]),
)
D_PEERS = sorted(range(1, NZ), key=lambda d: -ring(d, NZ))


def kernel(x_hbm, labels_ref, w_ref, grad_ref, step_ref, res_ref,
           xf, xh, xl, fbuf, dbuf, xsem, fs, fr, ds_, dr):
    feat = lax.axis_index("feat")
    z = lax.axis_index("dp")
    px, py, pc = feat // (NY * NC), (feat // NC) % NY, feat % NC

    loads = []
    for c in range(NCHUNK):
        rows = pl.ds(c * CHUNK, CHUNK)
        cp = pltpu.make_async_copy(x_hbm.at[rows], xf.at[rows], xsem.at[c])
        cp.start()
        loads.append(cp)

    def f_id(o):
        return {"feat": (((px + o[0]) % NX) * NY + (py + o[1]) % NY) * NC + (pc + o[2]) % NC}

    def d_id(o):
        return {"dp": (z + o) % NZ}

    barrier = pltpu.get_barrier_semaphore()
    for o in F_PEERS:
        pl.semaphore_signal(barrier, inc=1, device_id=f_id(o), device_id_type=MESH)
    for o in D_PEERS:
        pl.semaphore_signal(barrier, inc=1, device_id=d_id(o), device_id_type=MESH)

    sub = lax.broadcasted_iota(jnp.int32, (ROWS, LANES), 0)

    def lhs_of(v):
        hi = v.astype(jnp.bfloat16).astype(jnp.float32)
        lo = v - hi
        parts = []
        for k in range(ROWS):
            on = sub == k
            parts.append(jnp.concatenate([jnp.where(on, hi, 0.0), jnp.where(on, lo, 0.0)], axis=0).astype(jnp.bfloat16))
        return jnp.concatenate(parts, axis=1)

    def mult(lhs, rhs, dims):
        return lax.dot_general(lhs, rhs, (dims, ((), ())), preferred_element_type=jnp.float32)

    def to_slot(out, ref, base):
        total = jnp.sum(out, axis=0, keepdims=True)
        for k in range(out.shape[1] // LANES):
            ref[pl.ds(base + k, 1), :] = total[:, k * LANES:(k + 1) * LANES]

    def exchange(buf, n, me, count, rows, peers, ident, ssem, rsem, first=False):
        mine = buf.at[n, me, pl.ds(0, rows)]
        copies = []
        if first:
            pl.semaphore_wait(barrier, len(F_PEERS) + len(D_PEERS))
        for o in peers:
            cp = pltpu.make_async_remote_copy(
                src_ref=mine, dst_ref=mine, send_sem=ssem.at[n], recv_sem=rsem.at[n],
                device_id=ident(o), device_id_type=MESH)
            cp.start()
            copies.append(cp)
        some = buf.at[n, pl.ds(0, count - 1), pl.ds(0, rows)]
        pltpu.make_async_copy(some, some, rsem.at[n]).wait()
        return some, ssem.at[n]

    def summed(buf, n, count, lo, hi):
        parts = [buf[n, k, pl.ds(lo, hi - lo), :] for k in range(count)]
        while len(parts) > 1:
            parts = [parts[i] + parts[i + 1] for i in range(0, len(parts), 2)]
        return parts[0]

    sent = []
    lhs = lhs_of(w_ref[...])
    for c in range(NCHUNK):
        loads[c].wait()
        rows = pl.ds(c * CHUNK, CHUNK)
        block = xf[rows, :]
        high = block.astype(jnp.bfloat16)
        low = (block - high.astype(jnp.float32)).astype(jnp.bfloat16)
        xh[rows, :] = high
        xl[rows, :] = low
        nt = ((1,), (1,))
        out = mult(lhs, high, nt) + mult(lhs, low, nt)
        to_slot(out, fbuf.at[0, feat], c * (CHUNK // LANES))
    sent.append(exchange(fbuf, 0, feat, NF, ROWS, F_PEERS, f_id, fs, fr, first=True))
    y = labels_ref[...].astype(jnp.float32)
    margin = y * summed(fbuf, 0, NF, 0, ROWS)
    sig = 1.0 / (1.0 + jnp.exp(-margin))
    curv = PENALTY * sig * (1.0 - sig)

    def back(u):
        lhs = lhs_of(u)
        nn = ((1,), (0,))
        return mult(lhs, xh[...], nn) + mult(lhs, xl[...], nn)

    def forward(v):
        lhs = lhs_of(v)
        nt = ((1,), (1,))
        return mult(lhs, xh[...], nt) + mult(lhs, xl[...], nt)

    to_slot(back((sig - 1.0) * y), dbuf.at[0, z], 0)
    sent.append(exchange(dbuf, 0, z, NZ, ROWS, D_PEERS, d_id, ds_, dr))
    gradient = w_ref[...] + PENALTY * summed(dbuf, 0, NZ, 0, ROWS)
    grad_ref[...] = gradient

    newton = jnp.zeros_like(gradient)
    residual = -gradient
    direction = residual
    image_rows = None
    rr = pp = None
    for step in range(1, CG_STEPS + 1):
        mine = fbuf.at[step, feat]
        to_slot(forward(residual), mine, 0)
        mine[pl.ds(ROWS, 1), :] = jnp.sum(residual * residual, axis=0, keepdims=True)
        if step > 1:
            mine[pl.ds(ROWS + 1, 1), :] = jnp.sum(residual * direction, axis=0, keepdims=True)
        nrows = ROWS + (1 if step == 1 else 2)
        sent.append(exchange(fbuf, step, feat, NF, nrows, F_PEERS, f_id, fs, fr))
        rows_r = summed(fbuf, step, NF, 0, ROWS)
        scal = jnp.sum(summed(fbuf, step, NF, ROWS, nrows), axis=1, keepdims=True)
        fresh = scal[0:1]
        if step == 1:
            image_rows = rows_r
            pp = fresh
        else:
            beta = fresh / rr
            direction = residual + beta * direction
            image_rows = rows_r + beta * image_rows
            pp = fresh + 2.0 * beta * scal[1:2] + beta * beta * pp
        rr = fresh
        weighted = curv * image_rows
        mine = dbuf.at[step, z]
        to_slot(back(weighted), mine, 0)
        mine[pl.ds(ROWS, 1), :] = jnp.sum(weighted * image_rows, axis=0, keepdims=True)
        sent.append(exchange(dbuf, step, z, NZ, ROWS + 1, D_PEERS, d_id, ds_, dr))
        image = direction + summed(dbuf, step, NZ, 0, ROWS)
        quad = jnp.sum(summed(dbuf, step, NZ, ROWS, ROWS + 1), axis=1, keepdims=True)
        alpha = rr / (pp + quad)
        newton = newton + alpha * direction
        residual = residual - alpha * image
    step_ref[...] = newton
    res_ref[...] = residual
    for some, sem in sent:
        pltpu.make_async_copy(some, some, sem).wait()


def local(features, labels, weights):
    vec = jax.ShapeDtypeStruct((ROWS, LANES), jnp.float32)
    vmem = pl.BlockSpec(memory_space=pltpu.VMEM)
    outs = pl.pallas_call(
        kernel,
        name="newton_cg",
        out_shape=(vec, vec, vec),
        in_specs=[pl.BlockSpec(memory_space=pltpu.HBM), vmem, vmem],
        out_specs=(vmem, vmem, vmem),
        scratch_shapes=[
            pltpu.VMEM((N, N), jnp.float32),
            pltpu.VMEM((N, N), jnp.bfloat16),
            pltpu.VMEM((N, N), jnp.bfloat16),
            pltpu.VMEM((CG_STEPS + 1, NF, SLOT, LANES), jnp.float32),
            pltpu.VMEM((CG_STEPS + 1, NZ, SLOT, LANES), jnp.float32),
            pltpu.SemaphoreType.DMA((NCHUNK,)),
            pltpu.SemaphoreType.DMA((CG_STEPS + 1,)),
            pltpu.SemaphoreType.DMA((CG_STEPS + 1,)),
            pltpu.SemaphoreType.DMA((CG_STEPS + 1,)),
            pltpu.SemaphoreType.DMA((CG_STEPS + 1,)),
        ],
        compiler_params=pltpu.CompilerParams(
            collective_id=0, has_side_effects=True, vmem_limit_bytes=62 * 1024 * 1024
        ),
    )(features, labels.reshape(ROWS, LANES), weights.reshape(ROWS, LANES))
    return tuple(o.reshape(N) for o in outs)


def solution(mesh):
    placed = (P("dp", "feat"), P("dp"), P("feat"))
    return jax.shard_map(
        local,
        mesh=mesh,
        in_specs=placed,
        out_specs=(P("feat"), P("feat"), P("feat")),
        check_vma=False,
    )
```

```python
import functools

import jax
import jax.numpy as jnp
from jax import lax
from jax.experimental import pallas as pl
from jax.experimental.pallas import tpu as pltpu
from jax.sharding import PartitionSpec as P

CG_STEPS = 3
PENALTY = 4.0
MESH = pl.DeviceIdType.MESH

N = 1024
LANES = 128
ROWS = N // LANES
CHUNK = 256
NCHUNK = N // CHUNK
NX, NY, NC, NZ = 4, 4, 2, 8
NF = NX * NY * NC
SLOT = 16


def ring(d, n):
    return min(d, n - d)


F_PEERS = sorted(
    ((a, b, c) for a in range(NX) for b in range(NY) for c in range(NC) if (a, b, c) != (0, 0, 0)),
    key=lambda o: (-(ring(o[0], NX) + ring(o[1], NY)), -o[2]),
)
D_PEERS = sorted(range(1, NZ), key=lambda d: -ring(d, NZ))


def kernel(x_hbm, labels_hbm, w_hbm, out_ref,
           xf, xh, xl, labels_ref, w_ref, fbuf, dbuf, vsem, xsem, fs, fr, ds_, dr):
    feat = lax.axis_index("feat")
    z = lax.axis_index("dp")
    px, py, pc = feat // (NY * NC), (feat // NC) % NY, feat % NC

    w_load = pltpu.make_async_copy(w_hbm, w_ref, vsem.at[0])
    w_load.start()
    loads = []
    for c in range(NCHUNK):
        rows = pl.ds(c * CHUNK, CHUNK)
        cp = pltpu.make_async_copy(x_hbm.at[rows], xf.at[rows], xsem.at[c])
        cp.start()
        loads.append(cp)
    labels_load = pltpu.make_async_copy(labels_hbm, labels_ref, vsem.at[1])
    labels_load.start()

    def f_id(o):
        return {"feat": (((px + o[0]) % NX) * NY + (py + o[1]) % NY) * NC + (pc + o[2]) % NC}

    def d_id(o):
        return {"dp": (z + o) % NZ}

    barrier = pltpu.get_barrier_semaphore()
    for o in F_PEERS:
        pl.semaphore_signal(barrier, inc=1, device_id=f_id(o), device_id_type=MESH)
    for o in D_PEERS:
        pl.semaphore_signal(barrier, inc=1, device_id=d_id(o), device_id_type=MESH)

    sub = lax.broadcasted_iota(jnp.int32, (ROWS, LANES), 0)

    def lhs_of(v):
        hi = v.astype(jnp.bfloat16).astype(jnp.float32)
        lo = v - hi
        parts = []
        for k in range(ROWS):
            on = sub == k
            parts.append(jnp.concatenate([jnp.where(on, hi, 0.0), jnp.where(on, lo, 0.0)], axis=0).astype(jnp.bfloat16))
        return jnp.concatenate(parts, axis=1)

    def mult(lhs, rhs, dims):
        return lax.dot_general(lhs, rhs, (dims, ((), ())), preferred_element_type=jnp.float32)

    def to_slot(out, ref, base):
        total = jnp.sum(out, axis=0, keepdims=True)
        for k in range(out.shape[1] // LANES):
            ref[pl.ds(base + k, 1), :] = total[:, k * LANES:(k + 1) * LANES]

    def exchange(buf, n, me, count, rows, peers, ident, ssem, rsem, first=False):
        mine = buf.at[n, me, pl.ds(0, rows)]
        copies = []
        if first:
            pl.semaphore_wait(barrier, len(F_PEERS) + len(D_PEERS))
        for o in peers:
            cp = pltpu.make_async_remote_copy(
                src_ref=mine, dst_ref=mine, send_sem=ssem.at[n], recv_sem=rsem.at[n],
                device_id=ident(o), device_id_type=MESH)
            cp.start()
            copies.append(cp)
        some = buf.at[n, pl.ds(0, count - 1), pl.ds(0, rows)]
        pltpu.make_async_copy(some, some, rsem.at[n]).wait()
        return some, ssem.at[n]

    def summed(buf, n, count, lo, hi):
        parts = [buf[n, k, pl.ds(lo, hi - lo), :] for k in range(count)]
        while len(parts) > 1:
            parts = [parts[i] + parts[i + 1] for i in range(0, len(parts), 2)]
        return parts[0]

    sent = []
    w_load.wait()
    lhs = lhs_of(w_ref[...])
    for c in range(NCHUNK):
        loads[c].wait()
        rows = pl.ds(c * CHUNK, CHUNK)
        block = xf[rows, :]
        high = block.astype(jnp.bfloat16)
        low = (block - high.astype(jnp.float32)).astype(jnp.bfloat16)
        xh[rows, :] = high
        xl[rows, :] = low
        nt = ((1,), (1,))
        out = mult(lhs, high, nt) + mult(lhs, low, nt)
        to_slot(out, fbuf.at[0, feat], c * (CHUNK // LANES))
    sent.append(exchange(fbuf, 0, feat, NF, ROWS, F_PEERS, f_id, fs, fr, first=True))
    labels_load.wait()
    y = labels_ref[...].astype(jnp.float32)
    margin = y * summed(fbuf, 0, NF, 0, ROWS)
    sig = 1.0 / (1.0 + jnp.exp(-margin))
    curv = PENALTY * sig * (1.0 - sig)

    def back(u):
        lhs = lhs_of(u)
        nn = ((1,), (0,))
        return mult(lhs, xh[...], nn) + mult(lhs, xl[...], nn)

    def forward(v):
        lhs = lhs_of(v)
        nt = ((1,), (1,))
        return mult(lhs, xh[...], nt) + mult(lhs, xl[...], nt)

    to_slot(back((sig - 1.0) * y), dbuf.at[0, z], 0)
    sent.append(exchange(dbuf, 0, z, NZ, ROWS, D_PEERS, d_id, ds_, dr))
    gradient = w_ref[...] + PENALTY * summed(dbuf, 0, NZ, 0, ROWS)
    out_ref[0:8] = gradient

    newton = jnp.zeros_like(gradient)
    residual = -gradient
    direction = residual
    image_rows = None
    rr = pp = None
    for step in range(1, CG_STEPS + 1):
        mine = fbuf.at[step, feat]
        to_slot(forward(residual), mine, 0)
        mine[pl.ds(ROWS, 1), :] = jnp.sum(residual * residual, axis=0, keepdims=True)
        if step > 1:
            mine[pl.ds(ROWS + 1, 1), :] = jnp.sum(residual * direction, axis=0, keepdims=True)
        nrows = ROWS + (1 if step == 1 else 2)
        sent.append(exchange(fbuf, step, feat, NF, nrows, F_PEERS, f_id, fs, fr))
        rows_r = summed(fbuf, step, NF, 0, ROWS)
        scal = jnp.sum(summed(fbuf, step, NF, ROWS, nrows), axis=1, keepdims=True)
        fresh = scal[0:1]
        if step == 1:
            image_rows = rows_r
            pp = fresh
        else:
            beta = fresh / rr
            direction = residual + beta * direction
            image_rows = rows_r + beta * image_rows
            pp = fresh + 2.0 * beta * scal[1:2] + beta * beta * pp
        rr = fresh
        weighted = curv * image_rows
        mine = dbuf.at[step, z]
        to_slot(back(weighted), mine, 0)
        mine[pl.ds(ROWS, 1), :] = jnp.sum(weighted * image_rows, axis=0, keepdims=True)
        sent.append(exchange(dbuf, step, z, NZ, ROWS + 1, D_PEERS, d_id, ds_, dr))
        image = direction + summed(dbuf, step, NZ, 0, ROWS)
        quad = jnp.sum(summed(dbuf, step, NZ, ROWS, ROWS + 1), axis=1, keepdims=True)
        alpha = rr / (pp + quad)
        newton = newton + alpha * direction
        residual = residual - alpha * image
    out_ref[8:16] = newton
    out_ref[16:24] = residual
    for some, sem in sent:
        pltpu.make_async_copy(some, some, sem).wait()


def local(features, labels, weights):
    vmem = pl.BlockSpec(memory_space=pltpu.VMEM)
    hbm = pl.BlockSpec(memory_space=pltpu.HBM)
    outs = pl.pallas_call(
        kernel,
        name="newton_cg",
        out_shape=pltpu.VMEM((3*ROWS, LANES), jnp.float32),
        in_specs=[hbm, hbm, hbm],
        out_specs=vmem,
        scratch_shapes=[
            pltpu.VMEM((N, N), jnp.float32),
            pltpu.VMEM((N, N), jnp.bfloat16),
            pltpu.VMEM((N, N), jnp.bfloat16),
            pltpu.VMEM((ROWS, LANES), jnp.int32),
            pltpu.VMEM((ROWS, LANES), jnp.float32),
            pltpu.VMEM((CG_STEPS + 1, NF, SLOT, LANES), jnp.float32),
            pltpu.VMEM((CG_STEPS + 1, NZ, SLOT, LANES), jnp.float32),
            pltpu.SemaphoreType.DMA((2,)),
            pltpu.SemaphoreType.DMA((NCHUNK,)),
            pltpu.SemaphoreType.DMA((CG_STEPS + 1,)),
            pltpu.SemaphoreType.DMA((CG_STEPS + 1,)),
            pltpu.SemaphoreType.DMA((CG_STEPS + 1,)),
            pltpu.SemaphoreType.DMA((CG_STEPS + 1,)),
        ],
        compiler_params=pltpu.CompilerParams(
            collective_id=0, has_side_effects=True, vmem_limit_bytes=62 * 1024 * 1024
        ),
    )(features, labels.reshape(ROWS, LANES), weights.reshape(ROWS, LANES))
    outs = outs.reshape(3, N)
    return outs[0], outs[1], outs[2]


def solution(mesh):
    placed = (P("dp", "feat"), P("dp"), P("feat"))
    return jax.shard_map(
        local,
        mesh=mesh,
        in_specs=placed,
        out_specs=(P("feat"), P("feat"), P("feat")),
        check_vma=False,
    )
```
